32 devices in a mesh: row: 4 (over z), col: 8 (over y, x, core).
Axes of the slice: x: 2, y: 2, z: 4, core: 2. Of those that a mesh axis runs over, the one named last changes fastest.
Arguments:
- exchange_k: float32 [16, 16, 128, 128], P('row', 'col'), may hold values from -6 to 6
- margins: bfloat16 [16, 16, 2, 8, 128, 128], P('row', 'col'), may hold values from -0.5 to 0.5
- pno_energy: float32 [16, 16, 128], P('row', 'col'), may hold values from 0.4 to 4
- pno_count: int32 [16, 16], P('row', 'col'), may hold values from 64 to 128
- occ_energy: float32 [16], replicated, may hold values from -1.5 to -0.3
- coupling: float32 [16, 8], replicated, may hold values from -0.15 to 0.15
- neighbours: int32 [16, 8], replicated, may hold values from 0 to 15, as said below
Outputs:
- amplitudes: float32 [16, 16, 128, 128], P('row', 'col')
- residual: float32 [16, 16, 128, 128], P('row', 'col')
The draws below stay inside these ranges and needn't reach their ends.
Inputs may be any that keep to these rules, and one draw needn't show every extreme that they name: `neighbours`: row i lists 8 different orbitals k, none equal to i, each within 6 positions of i counted cyclically modulo 16.
All inputs are finite; a program needn't handle non-finite values.
Results may differ from the reference program's by a relative error of at most 0.00045.
Values may be sent and summed in bfloat16 or wider, within the bound.
A program may use at most 128 MiB of HBM per device.

```python
import math
import jax
import jax.numpy as jnp
from jax import lax

PNO = 128
NBR = 8
REACH = 6
ITERS = 3
NOCC = 16


def draw_neighbours(key, part):
    owners = jnp.arange(NOCC, dtype=jnp.int32)
    row_keys = jax.random.split(jax.random.fold_in(key, 11), NOCC)
    picks = jax.vmap(lambda row_key: jax.random.permutation(row_key, 2 * REACH)[:NBR])(row_keys)
    picks = picks.astype(jnp.int32)
    offsets = jnp.where(picks < REACH, picks - REACH, picks - REACH + 1)
    return ((owners[:, None] + offsets + NOCC) % NOCC).astype(jnp.int32)


def set_ends(drawn, rng, low, top_value):
    index_at = [jax.random.randint(jax.random.fold_in(rng, axis), (), 0, length) for axis, length in enumerate(drawn.shape)]
    widest = drawn.shape.index(max(drawn.shape))
    beside = index_at[:widest] + [(index_at[widest] + 1) % drawn.shape[widest]] + index_at[widest + 1:]
    return drawn.at[tuple(index_at)].set(low).at[tuple(beside)].set(top_value)


def block_scale(key, extent, pieces, least, high):
    loudness = 1.0
    for axis_at, shards_of in pieces:
        heights = jax.random.uniform(jax.random.fold_in(jax.random.fold_in(key, 6), axis_at), (shards_of,), jnp.float32, least / len(pieces), high / len(pieces))
        loudness = loudness * jnp.repeat(jnp.exp(heights), extent[axis_at] // shards_of).reshape((-1,) + (1,) * (len(extent) - 1 - axis_at))
    return loudness


def normal_values(rng, shape, scale, limit, cuts=(), kind=jnp.bfloat16):
    array = scale * jax.random.normal(rng, shape, jnp.float32)
    if cuts:
        array = array * block_scale(rng, shape, cuts, -0.22, 0.18)
    return jnp.clip(array, -limit, limit).astype(kind)


def setup_inputs(seed: int = 0) -> dict:
    keys = jax.random.split(jax.random.key(seed), 8)
    exchange_k = normal_values(keys[0], (NOCC, NOCC, PNO, PNO), 1.0, 6.0, ((0, 4), (1, 8)), jnp.float32)
    margins = normal_values(keys[1], (NOCC, NOCC, 2, NBR, PNO, PNO), PNO ** -0.5, 0.5, ((0, 4), (1, 8)))
    pno_energy = jnp.clip(jnp.exp(math.log(4.0) - 2.3025851 * jax.random.uniform(keys[2], (NOCC, NOCC, PNO), jnp.float32) ** block_scale(keys[2], (NOCC, NOCC, PNO), ((0, 4), (1, 8)), -0.2, 0.2)), 0.4, 4.0)
    pno_count = set_ends(jax.random.randint(keys[3], (NOCC, NOCC), PNO // 2, PNO + 1), jax.random.fold_in(keys[3], 1), PNO // 2, PNO).astype(jnp.int32)
    occ_energy = jnp.clip(jax.random.uniform(keys[4], (NOCC,), jnp.float32, -1.5, -0.3), -1.5, -0.3)
    coupling = jnp.clip(jax.random.uniform(keys[5], (NOCC, NBR), jnp.float32, -0.15, 0.15), -0.15, 0.15)
    neighbours = draw_neighbours(jax.random.fold_in(keys[7], 71), 0)
    return {"exchange_k": exchange_k, "margins": margins, "pno_energy": pno_energy, "pno_count": pno_count, "occ_energy": occ_energy, "coupling": coupling, "neighbours": neighbours}


def two_sided(margin_pair, blocks, weights):
    half_way = jnp.einsum("jmab,jmbc->jmac", margin_pair.astype(jnp.float32), blocks.astype(jnp.float32)).astype(jnp.bfloat16)
    full_way = jnp.einsum("jmac,jmdc->jmad", half_way.astype(jnp.float32), margin_pair.astype(jnp.float32))
    return jnp.sum(full_way * weights[:, :, None, None], axis=1)


def reference(exchange_k, margins, pno_energy, pno_count, occ_energy, coupling, neighbours):
    levels = jnp.arange(PNO, dtype=jnp.int32)
    living = (levels[None, None, :] < pno_count[:, :, None]).astype(jnp.float32)
    pair_mask = living[:, :, :, None] * living[:, :, None, :]
    denominator = (pno_energy[:, :, :, None] + pno_energy[:, :, None, :]
                   - occ_energy[:, None, None, None] - occ_energy[None, :, None, None])
    amplitudes = jnp.zeros(exchange_k.shape, jnp.float32)
    residual = exchange_k
    for sweep_index in range(ITERS):
        if sweep_index > 0:
            rounded = amplitudes.astype(jnp.bfloat16)

            def one_row(orbital):
                margin_row = margins[orbital]
                near_rows = jnp.transpose(rounded[neighbours[orbital]], (1, 0, 2, 3))
                row_weights = jnp.broadcast_to(coupling[orbital][None, :], (NOCC, NBR))
                row_part = two_sided(margin_row[:, 0], near_rows, row_weights)
                near_cols = rounded[orbital][neighbours]
                col_part = two_sided(margin_row[:, 1], near_cols, coupling)
                return row_part + col_part

            coupled = lax.map(one_row, jnp.arange(NOCC, dtype=jnp.int32))
        else:
            coupled = jnp.zeros(exchange_k.shape, jnp.float32)
        residual = exchange_k + denominator * amplitudes - coupled
        updated = pair_mask * (amplitudes - residual / denominator)
        amplitudes = pair_mask * (0.5 * (updated + jnp.transpose(updated, (1, 0, 3, 2))))
    return amplitudes, residual
```

```python
import functools

import jax
import jax.numpy as jnp
from jax import lax
from jax.experimental import pallas as pl
from jax.experimental.pallas import tpu as pltpu
from jax.sharding import PartitionSpec as P

REACH = 6
ITERS = 3
MESH = pl.DeviceIdType.MESH
BF16 = jnp.bfloat16
F32 = jnp.float32


def spread(amount, peers):
    shards = -(-REACH // amount)
    whole = 2 * shards + 2 >= peers
    steps = [d for d in range(-shards, shards + 1) if d]
    if whole:
        steps = sorted({d % peers for d in steps})
    return whole, shards, steps


def flip(value, bit):
    return value + bit - 2 * bit * ((value // bit) % 2)


class Side:
    def __init__(self, amount, peers, me):
        self.amount, self.peers, self.me = amount, peers, me
        self.whole, self.shards, self.steps = spread(amount, peers)

    def slots(self):
        return (self.peers if self.whole else 2 * self.shards + 1) * self.amount

    def place(self, k):
        if self.whole:
            return k
        shard = lax.rem(k // self.amount - self.me + self.shards + self.peers, self.peers)
        return shard * self.amount + lax.rem(k, self.amount)

    def block(self, owner):
        return pl.ds(owner * self.amount, self.amount)

    def own(self):
        return self.me if self.whole else self.shards

    def landing(self, step):
        return self.me if self.whole else self.shards - step


def kernel(sizes, exch, marg_hbm, energy, count, occ, coupling, nbr, amp_out, res_out, *scratch):
    nr, nc, rows, cols, width, listed = sizes
    q = nr // nc
    sweeps = ITERS - 1
    scratch = list(scratch)
    marg, weight, denom, both, amps, coup, sent, mirrored = scratch[:8]
    del scratch[:8]
    row_bufs = [[scratch.pop(0) for _ in range(nc)] for _ in range(sweeps)]
    col_bufs = [[scratch.pop(0) for _ in range(nr)] for _ in range(sweeps)]
    marg_sem, mir_send, mir_recv, row_send, row_recv, col_send, col_recv = scratch

    r = lax.axis_index("row")
    c = lax.axis_index("col")
    rside, cside = Side(nr, rows, r), Side(nc, cols, c)
    ring = rside.whole and rows == 4 and nc % 2 == 0
    cube = cside.whole and cols == 8

    load = pltpu.make_async_copy(marg_hbm, marg, marg_sem)
    load.start()

    on_diagonal = c // q == r
    def partner(p):
        return (c // q, r * q + p)
    def is_self(p):
        return jnp.logical_and(on_diagonal, lax.rem(c, q) == p)
    def shift(step):
        return lax.rem(r + step + rows, rows)

    row_peers = [1, rows - 1] if ring else rside.steps
    if cube:
        col_peers = [flip(c, 1), flip(c, 2), flip(c, 4)]
    else:
        col_peers = [lax.rem(c + d + cols, cols) for d in cside.steps]
    barrier = pltpu.get_barrier_semaphore()
    for d in row_peers:
        pl.semaphore_signal(barrier, inc=1, device_id=(shift(d), c), device_id_type=MESH)
    for peer in col_peers:
        pl.semaphore_signal(barrier, inc=1, device_id=(r, peer), device_id_type=MESH)
    for p in range(q):
        @pl.when(jnp.logical_not(is_self(p)))
        def _():
            pl.semaphore_signal(barrier, inc=1, device_id=partner(p), device_id_type=MESH)

    def remote(src, dst, ssem, rsem, where):
        return pltpu.make_async_remote_copy(
            src_ref=src, dst_ref=dst, send_sem=ssem, recv_sem=rsem, device_id=where, device_id_type=MESH)

    def mirror_copy(phase, p, b):
        return remote(
            sent.at[phase, p, b], mirrored.at[phase, lax.rem(c, q), b],
            mir_send.at[phase, p, b], mir_recv.at[phase, lax.rem(c, q), b], partner(p))

    def mirror_arrival(phase, p, b):
        return remote(
            sent.at[phase, p, b], mirrored.at[phase, p, b],
            mir_send.at[phase, p, b], mir_recv.at[phase, p, b], partner(p))

    def mirror_start(phase, b):
        for p in range(q):
            @pl.when(jnp.logical_not(is_self(p)))
            def _():
                mirror_copy(phase, p, b).start()

            @pl.when(is_self(p))
            def _():
                mirrored[phase, p, b] = sent[phase, p, b]

    def mirror_wait(phase, b):
        for p in range(q):
            @pl.when(jnp.logical_not(is_self(p)))
            def _():
                mirror_arrival(phase, p, b).wait_recv()
                mirror_copy(phase, p, b).wait_send()

    line = lax.broadcasted_iota(jnp.int32, (width, width), 0)
    lane = lax.broadcasted_iota(jnp.int32, (width, width), 1)

    def prepare(i, b):
        e = jnp.broadcast_to(energy[i, pl.ds(b, 1), :], (width, width))
        d = e.T + e - occ[r * nr + i] - occ[c * nc + b]
        live = jnp.logical_and(line < count[i, b], lane < count[i, b])
        w = jnp.where(live, 1.0 / d, 0.0)
        g = exch[i, b] * w
        high = g.astype(BF16)
        weight[i, b] = w
        denom[i, b] = d
        both[i, b] = g
        coup[i, b] = jnp.zeros((width, width), F32)
        sent[0, i // nc, b, lax.rem(i, nc)] = high
        sent[1, i // nc, b, lax.rem(i, nc)] = (g - high.astype(F32)).astype(BF16)

    for b in range(nc):
        def body(i, carry):
            prepare(i, b)
            return carry
        lax.fori_loop(0, nr, body, 0)

    amount = len(row_peers) + len(col_peers) + q
    @pl.when(on_diagonal)
    def _():
        pl.semaphore_wait(barrier, amount - 1)
    @pl.when(jnp.logical_not(on_diagonal))
    def _():
        pl.semaphore_wait(barrier, amount)

    for phase in range(2):
        for b in range(nc):
            mirror_start(phase, b)

    def reflection(phase, i, j):
        return mirrored[phase, i // nc, lax.rem(i, nc), j].astype(F32).T

    def row_copy(s, j, which):
        buf = row_bufs[s][j]
        def one(owner, landing, step):
            return remote(buf.at[rside.block(owner)], buf.at[rside.block(landing)],
                          row_send.at[s, j, which], row_recv.at[s, j, which], (shift(step), c))
        if ring:
            if which == 0:
                return one(r, r, 1)
            if which == 1:
                return one(r, r, rows - 1)
            return one(shift(-1), shift(-1), 1) if j < nc // 2 else one(shift(1), shift(1), rows - 1)
        step = rside.steps[which]
        return one(rside.own(), rside.landing(step), step)

    def col_copy(s, i, which):
        buf = col_bufs[s][i]
        def one(owner, landing, peer):
            return remote(buf.at[cside.block(owner)], buf.at[cside.block(landing)],
                          col_send.at[s, i, which], col_recv.at[s, i, which], (r, peer))
        if cube:
            near, side, across = flip(c, 1), flip(c, 2), flip(c, 4)
            if which == 0:
                return one(c, c, side)
            if which == 1:
                return one(c, c, across)
            if which == 2:
                return one(side, side, across) if i < nr // 2 else one(across, across, side)
            block = (c, side, across, flip(side, 4))[which - 3]
            return one(block, block, near)
        step = cside.steps[which]
        return one(cside.own(), cside.landing(step), lax.rem(c + step + cols, cols))

    def col_first(s, i):
        for w in ((0, 1, 3) if cube else range(len(cside.steps))):
            col_copy(s, i, w).start()

    def row_first(s, j):
        for w in range(2 if ring else len(rside.steps)):
            row_copy(s, j, w).start()

    def col_second(s, i):
        if cube:
            for w in (0, 1):
                col_copy(s, i, w).wait_recv()
            for w in (2, 4, 5):
                col_copy(s, i, w).start()

    def col_third(s, i):
        if cube:
            col_copy(s, i, 2).wait_recv()
            col_copy(s, i, 6).start()

    def col_last(s, i):
        for w in (range(3, 7) if cube else range(len(cside.steps))):
            col_copy(s, i, w).wait_recv()

    def row_second(s, j):
        if ring:
            for w in (0, 1):
                row_copy(s, j, w).wait_recv()
            row_copy(s, j, 2).start()

    def row_last(s, j):
        for w in ((2,) if ring else range(len(rside.steps))):
            row_copy(s, j, w).wait_recv()

    def two_sided(buf, side, i, j, owner, place):
        halves, sides = [], []
        for m in range(listed):
            block = buf[place(nbr[owner, m])]
            s = marg[i, j, side, m]
            half = jnp.dot(s, block, preferred_element_type=F32) * coupling[owner, m]
            halves.append(half.astype(BF16))
            sides.append(s)
        full = lax.dot_general(
            jnp.concatenate(halves, axis=1), jnp.concatenate(sides, axis=1),
            (((1,), (1,)), ((), ())), preferred_element_type=F32)
        coup[i, j] = coup[i, j] + full

    def col_products(s, i):
        def body(j, carry):
            two_sided(col_bufs[s][i], 1, i, j, c * nc + j, cside.place)
            return carry
        lax.fori_loop(0, nc, body, 0)

    def row_products(s, j):
        def body(i, carry):
            two_sided(row_bufs[s][j], 0, i, j, r * nr + i, rside.place)
            return carry
        lax.fori_loop(0, nr, body, 0)

    def own_slot(side, local):
        return side.own() * side.amount + local

    for s in range(sweeps):
        for b in range(nc):
            mirror_wait(0 if s == 0 else s + 1, b)
        for i in range(nr):
            for j in range(nc):
                if s == 0:
                    total = both[i, j] + reflection(0, i, j)
                    amp = jnp.where(weight[i, j] != 0.0, -0.5 * total, 0.0)
                else:
                    total = coup[i, j] * weight[i, j] + reflection(s + 1, i, j) - both[i, j]
                    amp = jnp.where(weight[i, j] != 0.0, 0.5 * total, 0.0)
                    coup[i, j] = jnp.zeros((width, width), F32)
                if s == sweeps - 1:
                    amps[i, j] = amp
                small = amp.astype(BF16)
                row_bufs[s][j][own_slot(rside, i)] = small
                col_bufs[s][i][own_slot(cside, j)] = small
            col_first(s, i)
        for j in range(nc):
            row_first(s, j)
        if s == 0:
            load.wait()
            for b in range(nc):
                mirror_wait(1, b)
            for i in range(nr):
                for j in range(nc):
                    both[i, j] = both[i, j] + (reflection(0, i, j) + reflection(1, i, j))
        for t in range(nr + 2):
            if t < nr:
                col_second(s, t)
            if t < nc:
                row_second(s, t)
            if 1 <= t <= nr:
                col_third(s, t - 1)
            if t >= 2:
                col_last(s, t - 2)
                col_products(s, t - 2)
        for j in range(nc):
            row_last(s, j)
            row_products(s, j)
            for i in range(nr):
                sent[s + 2, i // nc, j, i % nc] = (coup[i, j] * weight[i, j]).astype(BF16)
            mirror_start(s + 2, j)

    for i in range(nr):
        for j in range(nc):
            res_out[i, j] = exch[i, j] + denom[i, j] * amps[i, j] - coup[i, j]
    for s in range(sweeps):
        for i in range(nr):
            for w in range(7 if cube else len(cside.steps)):
                col_copy(s, i, w).wait_send()
        for j in range(nc):
            for w in range(3 if ring else len(rside.steps)):
                row_copy(s, j, w).wait_send()
    for b in range(nc):
        mirror_wait(sweeps + 1, b)
    for i in range(nr):
        for j in range(nc):
            total = coup[i, j] * weight[i, j] + reflection(sweeps + 1, i, j) - both[i, j]
            amp_out[i, j] = jnp.where(weight[i, j] != 0.0, 0.5 * total, 0.0)


def per_device(rows, cols, exch, margins, energy, count, occ, coupling, nbr):
    nr, nc, width, _ = exch.shape
    listed = nbr.shape[1]
    sweeps = ITERS - 1
    q = nr // nc
    rside, cside = Side(nr, rows, 0), Side(nc, cols, 0)
    pairs = pltpu.VMEM((nr, nc, width, width), F32)
    mirror = pltpu.VMEM((sweeps + 2, q, nc, nc, width, width), BF16)
    dma = pltpu.SemaphoreType.DMA
    rsteps, csteps = max(3, len(rside.steps)), max(7, len(cside.steps))
    scratch = [pltpu.VMEM(margins.shape, BF16)] + [pairs] * 5 + [mirror] * 2
    scratch += [pltpu.VMEM((rside.slots(), width, width), BF16)] * (sweeps * nc)
    scratch += [pltpu.VMEM((cside.slots(), width, width), BF16)] * (sweeps * nr)
    scratch += [dma, dma((sweeps + 2, q, nc)), dma((sweeps + 2, q, nc))]
    scratch += [dma((sweeps, nc, rsteps))] * 2 + [dma((sweeps, nr, csteps))] * 2
    vmem = pl.BlockSpec(memory_space=pltpu.VMEM)
    smem = pl.BlockSpec(memory_space=pltpu.SMEM)
    return pl.pallas_call(
        functools.partial(kernel, (nr, nc, rows, cols, width, listed)),
        out_shape=(jax.ShapeDtypeStruct(exch.shape, F32), jax.ShapeDtypeStruct(exch.shape, F32)),
        in_specs=[vmem, pl.BlockSpec(memory_space=pl.ANY), vmem, smem, smem, smem, smem],
        out_specs=(vmem, vmem),
        scratch_shapes=scratch,
        compiler_params=pltpu.CompilerParams(
            collective_id=0, has_side_effects=True, vmem_limit_bytes=56 * 2**20),
        name="sweeps",
    )(exch, margins, energy, count, occ, coupling, nbr)


def solution(mesh):
    return jax.shard_map(
        functools.partial(per_device, mesh.shape["row"], mesh.shape["col"]),
        mesh=mesh,
        in_specs=(
            P("row", "col", None, None),
            P("row", "col", None, None, None, None),
            P("row", "col", None),
            P("row", "col"),
            P(),
            P(),
            P(),
        ),
        out_specs=(P("row", "col", None, None), P("row", "col", None, None)),
        check_vma=False,
    )
```

```python
import functools

import jax
import jax.numpy as jnp
from jax import lax
from jax.experimental import pallas as pl
from jax.experimental.pallas import tpu as pltpu
from jax.sharding import PartitionSpec as P

REACH = 6
ITERS = 3
MESH = pl.DeviceIdType.MESH
BF16 = jnp.bfloat16
F32 = jnp.float32


def spread(amount, peers):
    shards = -(-REACH // amount)
    whole = 2 * shards + 2 >= peers
    steps = [d for d in range(-shards, shards + 1) if d]
    if whole:
        steps = sorted({d % peers for d in steps})
    return whole, shards, steps


def flip(value, bit):
    return value + bit - 2 * bit * ((value // bit) % 2)


class Side:
    def __init__(self, amount, peers, me):
        self.amount, self.peers, self.me = amount, peers, me
        self.whole, self.shards, self.steps = spread(amount, peers)

    def slots(self):
        return (self.peers if self.whole else 2 * self.shards + 1) * self.amount

    def place(self, k):
        if self.whole:
            return k
        shard = lax.rem(k // self.amount - self.me + self.shards + self.peers, self.peers)
        return shard * self.amount + lax.rem(k, self.amount)

    def block(self, owner):
        return pl.ds(owner * self.amount, self.amount)

    def own(self):
        return self.me if self.whole else self.shards

    def landing(self, step):
        return self.me if self.whole else self.shards - step


def kernel(sizes, exch, marg_hbm, energy, count, occ, coupling, nbr, amp_out, res_out, *scratch):
    nr, nc, rows, cols, width, listed = sizes
    q = nr // nc
    sweeps = ITERS - 1
    scratch = list(scratch)
    marg, weight, denom, both, amps, coup, sent, mirrored = scratch[:8]
    del scratch[:8]
    row_bufs = [[scratch.pop(0) for _ in range(nc)] for _ in range(sweeps)]
    col_bufs = [[scratch.pop(0) for _ in range(nr)] for _ in range(sweeps)]
    marg_sem, mir_send, mir_recv, row_send, row_recv, col_send, col_recv = scratch

    r = lax.axis_index("row")
    c = lax.axis_index("col")
    rside, cside = Side(nr, rows, r), Side(nc, cols, c)
    ring = rside.whole and rows == 4 and nc % 2 == 0
    cube = cside.whole and cols == 8

    load = pltpu.make_async_copy(marg_hbm, marg, marg_sem)
    load.start()

    on_diagonal = c // q == r
    def partner(p):
        return (c // q, r * q + p)
    def is_self(p):
        return jnp.logical_and(on_diagonal, lax.rem(c, q) == p)
    def shift(step):
        return lax.rem(r + step + rows, rows)

    row_peers = [1, rows - 1] if ring else rside.steps
    if cube:
        col_peers = [flip(c, 1), flip(c, 2), flip(c, 4)]
    else:
        col_peers = [lax.rem(c + d + cols, cols) for d in cside.steps]
    barrier = pltpu.get_barrier_semaphore()
    for d in row_peers:
        pl.semaphore_signal(barrier, inc=1, device_id=(shift(d), c), device_id_type=MESH)
    for peer in col_peers:
        pl.semaphore_signal(barrier, inc=1, device_id=(r, peer), device_id_type=MESH)
    for p in range(q):
        @pl.when(jnp.logical_not(is_self(p)))
        def _():
            pl.semaphore_signal(barrier, inc=1, device_id=partner(p), device_id_type=MESH)

    def remote(src, dst, ssem, rsem, where):
        return pltpu.make_async_remote_copy(
            src_ref=src, dst_ref=dst, send_sem=ssem, recv_sem=rsem, device_id=where, device_id_type=MESH)

    def mirror_copy(phase, p, b):
        return remote(
            sent.at[phase, p, b], mirrored.at[phase, lax.rem(c, q), b],
            mir_send.at[phase, p, b], mir_recv.at[phase, lax.rem(c, q), b], partner(p))

    def mirror_arrival(phase, p, b):
        return remote(
            sent.at[phase, p, b], mirrored.at[phase, p, b],
            mir_send.at[phase, p, b], mir_recv.at[phase, p, b], partner(p))

    def mirror_start(phase, b):
        for p in range(q):
            @pl.when(jnp.logical_not(is_self(p)))
            def _():
                mirror_copy(phase, p, b).start()

            @pl.when(is_self(p))
            def _():
                mirrored[phase, p, b] = sent[phase, p, b]

    def mirror_wait(phase, b):
        for p in range(q):
            @pl.when(jnp.logical_not(is_self(p)))
            def _():
                mirror_arrival(phase, p, b).wait_recv()
                mirror_copy(phase, p, b).wait_send()

    line = lax.broadcasted_iota(jnp.int32, (width, width), 0)
    lane = lax.broadcasted_iota(jnp.int32, (width, width), 1)

    def prepare(i, b):
        e = jnp.broadcast_to(energy[i, pl.ds(b, 1), :], (width, width))
        d = e.T + e - occ[r * nr + i] - occ[c * nc + b]
        live = jnp.logical_and(line < count[i, b], lane < count[i, b])
        w = jnp.where(live, 1.0 / d, 0.0)
        g = exch[i, b] * w
        high = g.astype(BF16)
        weight[i, b] = w
        denom[i, b] = d
        both[i, b] = g
        coup[i, b] = jnp.zeros((width, width), F32)
        sent[0, i // nc, b, lax.rem(i, nc)] = high
        sent[1, i // nc, b, lax.rem(i, nc)] = (g - high.astype(F32)).astype(BF16)

    for b in range(nc):
        def body(i, carry):
            prepare(i, b)
            return carry
        lax.fori_loop(0, nr, body, 0)

    amount = len(row_peers) + len(col_peers) + q
    @pl.when(on_diagonal)
    def _():
        pl.semaphore_wait(barrier, amount - 1)
    @pl.when(jnp.logical_not(on_diagonal))
    def _():
        pl.semaphore_wait(barrier, amount)

    for b in range(nc):
        mirror_start(0, b)

    def reflection(phase, i, j):
        return mirrored[phase, i // nc, lax.rem(i, nc), j].astype(F32).T

    def row_copy(s, j, which):
        buf = row_bufs[s][j]
        def one(owner, landing, step):
            return remote(buf.at[rside.block(owner)], buf.at[rside.block(landing)],
                          row_send.at[s, j, which], row_recv.at[s, j, which], (shift(step), c))
        if ring:
            if which == 0:
                return one(r, r, 1)
            if which == 1:
                return one(r, r, rows - 1)
            return one(shift(-1), shift(-1), 1) if j < nc // 2 else one(shift(1), shift(1), rows - 1)
        step = rside.steps[which]
        return one(rside.own(), rside.landing(step), step)

    def col_copy(s, i, which):
        buf = col_bufs[s][i]
        def one(owner, landing, peer):
            return remote(buf.at[cside.block(owner)], buf.at[cside.block(landing)],
                          col_send.at[s, i, which], col_recv.at[s, i, which], (r, peer))
        if cube:
            near, side, across = flip(c, 1), flip(c, 2), flip(c, 4)
            if which == 0:
                return one(c, c, side)
            if which == 1:
                return one(c, c, across)
            if which == 2:
                return one(side, side, across) if i < nr // 2 else one(across, across, side)
            block = (c, side, across, flip(side, 4))[which - 3]
            return one(block, block, near)
        step = cside.steps[which]
        return one(cside.own(), cside.landing(step), lax.rem(c + step + cols, cols))

    def col_first(s, i):
        for w in ((0, 1, 3) if cube else range(len(cside.steps))):
            col_copy(s, i, w).start()

    def row_first(s, j):
        for w in range(2 if ring else len(rside.steps)):
            row_copy(s, j, w).start()

    def col_second(s, i):
        if cube:
            for w in (0, 1):
                col_copy(s, i, w).wait_recv()
            for w in (2, 4, 5):
                col_copy(s, i, w).start()

    def col_third(s, i):
        if cube:
            col_copy(s, i, 2).wait_recv()
            col_copy(s, i, 6).start()

    def col_last(s, i):
        for w in (range(3, 7) if cube else range(len(cside.steps))):
            col_copy(s, i, w).wait_recv()

    def row_second(s, j):
        if ring:
            for w in (0, 1):
                row_copy(s, j, w).wait_recv()
            row_copy(s, j, 2).start()

    def row_last(s, j):
        for w in ((2,) if ring else range(len(rside.steps))):
            row_copy(s, j, w).wait_recv()

    def two_sided(buf, side, i, j, owner, place):
        halves, sides = [], []
        for m in range(listed):
            block = buf[place(nbr[owner, m])]
            s = marg[i, j, side, m]
            half = jnp.dot(s, block, preferred_element_type=F32) * coupling[owner, m]
            halves.append(half.astype(BF16))
            sides.append(s)
        full = lax.dot_general(
            jnp.concatenate(halves, axis=1), jnp.concatenate(sides, axis=1),
            (((1,), (1,)), ((), ())), preferred_element_type=F32)
        coup[i, j] = coup[i, j] + full

    def col_products(s, i):
        def body(j, carry):
            two_sided(col_bufs[s][i], 1, i, j, c * nc + j, cside.place)
            return carry
        lax.fori_loop(0, nc, body, 0, unroll=True)

    def row_products(s, j):
        def body(i, carry):
            two_sided(row_bufs[s][j], 0, i, j, r * nr + i, rside.place)
            return carry
        lax.fori_loop(0, nr, body, 0, unroll=2)

    def own_slot(side, local):
        return side.own() * side.amount + local

    for s in range(sweeps):
        for b in range(nc):
            mirror_wait(0 if s == 0 else s + 1, b)
        for i in range(nr):
            for j in range(nc):
                if s == 0:
                    total = both[i, j] + reflection(0, i, j)
                    amp = jnp.where(weight[i, j] != 0.0, -0.5 * total, 0.0)
                else:
                    total = coup[i, j] * weight[i, j] + reflection(s + 1, i, j) - both[i, j]
                    amp = jnp.where(weight[i, j] != 0.0, 0.5 * total, 0.0)
                    coup[i, j] = jnp.zeros((width, width), F32)
                if s == sweeps - 1:
                    amps[i, j] = amp
                small = amp.astype(BF16)
                row_bufs[s][j][own_slot(rside, i)] = small
                col_bufs[s][i][own_slot(cside, j)] = small
            col_first(s, i)
        for j in range(nc):
            row_first(s, j)
        if s == 0:
            load.wait()
            for i in range(nr):
                for j in range(nc):
                    both[i, j] = both[i, j] + reflection(0, i, j)
        for t in range(nr + 2):
            if t < nr:
                col_second(s, t)
            if t < nc:
                row_second(s, t)
            if 1 <= t <= nr:
                col_third(s, t - 1)
            if t >= 2:
                col_last(s, t - 2)
                col_products(s, t - 2)
        if s == 0:
            for b in range(nc):
                mirror_start(1, b)
        for j in range(nc):
            row_last(s, j)
            row_products(s, j)
            for i in range(nr):
                sent[s + 2, i // nc, j, i % nc] = (coup[i, j] * weight[i, j]).astype(BF16)
            mirror_start(s + 2, j)
        if s == 0:
            for b in range(nc):
                mirror_wait(1, b)
            for i in range(nr):
                for j in range(nc):
                    both[i, j] = both[i, j] + reflection(1, i, j)

    for i in range(nr):
        for j in range(nc):
            res_out[i, j] = exch[i, j] + denom[i, j] * amps[i, j] - coup[i, j]
    for s in range(sweeps):
        for i in range(nr):
            for w in range(7 if cube else len(cside.steps)):
                col_copy(s, i, w).wait_send()
        for j in range(nc):
            for w in range(3 if ring else len(rside.steps)):
                row_copy(s, j, w).wait_send()
    for b in range(nc):
        mirror_wait(sweeps + 1, b)
    for i in range(nr):
        for j in range(nc):
            total = coup[i, j] * weight[i, j] + reflection(sweeps + 1, i, j) - both[i, j]
            amp_out[i, j] = jnp.where(weight[i, j] != 0.0, 0.5 * total, 0.0)


def per_device(rows, cols, exch, margins, energy, count, occ, coupling, nbr):
    nr, nc, width, _ = exch.shape
    listed = nbr.shape[1]
    sweeps = ITERS - 1
    q = nr // nc
    rside, cside = Side(nr, rows, 0), Side(nc, cols, 0)
    pairs = pltpu.VMEM((nr, nc, width, width), F32)
    mirror = pltpu.VMEM((sweeps + 2, q, nc, nc, width, width), BF16)
    dma = pltpu.SemaphoreType.DMA
    rsteps, csteps = max(3, len(rside.steps)), max(7, len(cside.steps))
    scratch = [pltpu.VMEM(margins.shape, BF16)] + [pairs] * 5 + [mirror] * 2
    scratch += [pltpu.VMEM((rside.slots(), width, width), BF16)] * (sweeps * nc)
    scratch += [pltpu.VMEM((cside.slots(), width, width), BF16)] * (sweeps * nr)
    scratch += [dma, dma((sweeps + 2, q, nc)), dma((sweeps + 2, q, nc))]
    scratch += [dma((sweeps, nc, rsteps))] * 2 + [dma((sweeps, nr, csteps))] * 2
    vmem = pl.BlockSpec(memory_space=pltpu.VMEM)
    smem = pl.BlockSpec(memory_space=pltpu.SMEM)
    return pl.pallas_call(
        functools.partial(kernel, (nr, nc, rows, cols, width, listed)),
        out_shape=(jax.ShapeDtypeStruct(exch.shape, F32), jax.ShapeDtypeStruct(exch.shape, F32)),
        in_specs=[vmem, pl.BlockSpec(memory_space=pl.ANY), vmem, smem, smem, smem, smem],
        out_specs=(vmem, vmem),
        scratch_shapes=scratch,
        compiler_params=pltpu.CompilerParams(
            collective_id=0, has_side_effects=True, vmem_limit_bytes=56 * 2**20),
        name="sweeps",
    )(exch, margins, energy, count, occ, coupling, nbr)


def solution(mesh):
    return jax.shard_map(
        functools.partial(per_device, mesh.shape["row"], mesh.shape["col"]),
        mesh=mesh,
        in_specs=(
            P("row", "col", None, None),
            P("row", "col", None, None, None, None),
            P("row", "col", None),
            P("row", "col"),
            P(),
            P(),
            P(),
        ),
        out_specs=(P("row", "col", None, None), P("row", "col", None, None)),
        check_vma=False,
    )
```
